256 devices in a mesh: dp: 64 (over x_lo, z, y), tensor: 4 (over x_hi, core).
Axes of the slice: x: 4 (x_hi: 2, x_lo: 2; x = x_hi * 2 + x_lo), y: 4, z: 8, core: 2. Of those that a mesh axis runs over, the one named last changes fastest.
Arguments:
- attn_out: bfloat16 [16384, 4096], P('dp', 'tensor'), may hold values from -6 to 6
- w_blocks: bfloat16 [4096, 8192], P('tensor', 'dp'), may hold values from -0.09375 to 0.09375
- w_scales: float32 [32, 8192], P('tensor', 'dp'), may hold values from 0.5 to 2
- residual: bfloat16 [16384, 8192], P('dp')
- gain: float32 [8192], P('tensor'), may hold values from 0.5 to 1.5
Outputs:
- hidden: bfloat16 [16384, 8192], P('dp', 'tensor')
- normed: bfloat16 [16384, 8192], P('dp', 'tensor')
The draws below stay inside these ranges and needn't reach their ends.
All inputs are finite; a program needn't handle non-finite values.
Results may differ from the reference program's by a relative error of at most 0.014.
Values may be sent and summed in bfloat16 or wider, within the bound.
No kernel may reach another device: no remote copies, remote signals or barrier semaphores. Data moves between devices by JAX's collectives and lax.ppermute only.
A program may use at most 128 MiB of HBM per device.

```python
import math
import jax
import jax.numpy as jnp
from jax import lax

D = 8192
BLOCK = 128
HD = 4096
TOKENS = 16384


def draw_residual(key, part):
    first = jax.random.fold_in(jax.random.fold_in(key, 17), 0)
    base = jnp.clip(jax.random.normal(first, (TOKENS, D), jnp.float32), -6.0, 6.0)
    ramp = 0.6 * jnp.exp(math.log(3.0) * jnp.arange(D, dtype=jnp.float32) / D)
    return (base * ramp[None, :]).astype(jnp.bfloat16)


def shard_levels(rng, extent, shards, smallest, high):
    level, own = 1.0, jax.random.fold_in(rng, 6)
    for dim, parts in shards:
        heights = jnp.exp(jax.random.uniform(jax.random.fold_in(own, dim), (parts,), jnp.float32, smallest / len(shards), high / len(shards)))
        level = level * jnp.repeat(heights, extent[dim] // parts).reshape([-1 if axis == dim else 1 for axis in range(len(extent))])
    return level


def bell_draw(own_key, shape, scale, most, cuts=(), held_as=jnp.bfloat16):
    values = jax.random.normal(own_key, shape, jnp.float32) * scale
    if len(cuts) > 0:
        values = shard_levels(own_key, shape, cuts, -0.22, 0.18) * values
    return jnp.clip(values, min=-most, max=most).astype(held_as)


def setup_inputs(seed: int = 0) -> dict:
    key_list = jax.random.split(jax.random.key(seed), 6)
    attn_out = bell_draw(key_list[0], (TOKENS, HD), 1.0, 6.0, ((0, 64), (1, 4)))
    w_blocks = bell_draw(key_list[1], (HD, D), HD ** -0.5, 0.09375, ((0, 4), (1, 64)))
    w_scales = jnp.clip(jnp.exp(math.log(2.0) - 1.3862944 * jax.random.uniform(key_list[2], (HD // BLOCK, D), jnp.float32) ** shard_levels(key_list[2], (HD // BLOCK, D), ((0, 4), (1, 64)), -0.2, 0.2)), 0.5, 2.0)
    residual = draw_residual(jax.random.fold_in(key_list[5], 71), 0)
    gain = jnp.clip(1.0 + 0.1 * jax.random.normal(key_list[4], (D,), jnp.float32), 0.5, 1.5)
    return {"attn_out": attn_out, "w_blocks": w_blocks, "w_scales": w_scales, "residual": residual, "gain": gain}


def dequantize(blocks, scales):
    spread = jnp.repeat(scales, BLOCK, axis=0)
    return (blocks.astype(jnp.float32) * spread).astype(jnp.bfloat16)

def reference(attn_out, w_blocks, w_scales, residual, gain):
    weights = dequantize(w_blocks, w_scales)
    attn_sum = jnp.dot(attn_out, weights, preferred_element_type=jnp.float32)
    hidden = (residual.astype(jnp.float32) + attn_sum).astype(jnp.bfloat16)
    wide = hidden.astype(jnp.float32)
    mean_square = lax.optimization_barrier(jnp.sum(wide * wide, axis=1, keepdims=True)) / D
    normed = (wide * gain[None, :] * jax.lax.rsqrt(mean_square + 1e-05)).astype(jnp.bfloat16)
    return (hidden, normed)
```

```python
import jax
import jax.numpy as jnp
from jax import lax
from jax.experimental import pallas as pl
from jax.experimental.pallas import tpu as pltpu
from jax.sharding import PartitionSpec as P

BLOCK = 128
XL, Z, Y, XH, CORE = 2, 8, 4, 2, 2


def move(x, where):
    pairs = []
    for xl in range(XL):
        for z in range(Z):
            for y in range(Y):
                for xh in range(XH):
                    for core in range(CORE):
                        to = where(xl, z, y, xh, core)
                        if to is None:
                            continue
                        xl2, z2, y2, xh2, core2 = to
                        source = ((xl * Z + z) * Y + y) * 4 + xh * 2 + core
                        target = ((xl2 * Z + z2 % Z) * Y + y2 % Y) * 4 + xh2 * 2 + core2
                        pairs.append((source, target))
    return lax.ppermute(x, ("dp", "tensor"), pairs)


def dequantize(blocks, scales):
    rows, cols = blocks.shape
    shaped = blocks.astype(jnp.float32).reshape(rows // BLOCK, BLOCK, cols)
    return (shaped * scales[:, None, :]).reshape(rows, cols).astype(jnp.bfloat16)


def vmem(count):
    return [pl.BlockSpec(memory_space=pltpu.VMEM)] * count


def smem():
    return pl.BlockSpec(memory_space=pltpu.SMEM)


def project_kernel(slot_ref, *refs):
    acts_own, acts_other = refs[0:4], refs[4:8]
    w_own, w_other = refs[8:16], refs[16:24]
    keep_ref, send_ref, acts, weights = refs[24:28]
    tokens, depth = acts_own[0].shape
    for k in range(Z):
        cols = pl.ds(pl.multiple_of(slot_ref[k] * BLOCK, BLOCK), BLOCK)
        weights[0:depth, cols] = w_own[k][...]
        weights[depth : 2 * depth, cols] = w_other[k][...]
    for j in range(Y):
        rows = slice(j * tokens, (j + 1) * tokens)
        acts[rows, 0:depth] = acts_own[j][...]
        acts[rows, depth : 2 * depth] = acts_other[j][...]
    half = keep_ref.shape[1]
    for n in range(0, half, 256):
        keep_ref[:, n : n + 256] = jnp.dot(
            acts[...], weights[:, n : n + 256], preferred_element_type=jnp.float32
        )
    for n in range(0, half, 256):
        send_ref[:, n : n + 256] = jnp.dot(
            acts[...], weights[:, half + n : half + n + 256], preferred_element_type=jnp.float32
        ).astype(jnp.bfloat16)


def project(slots, acts_own, acts_other, w_own, w_other):
    tokens, depth = acts_own[0].shape
    half = Z * BLOCK // 2
    return pl.pallas_call(
        project_kernel,
        out_shape=(
            jax.ShapeDtypeStruct((Y * tokens, half), jnp.float32),
            jax.ShapeDtypeStruct((Y * tokens, half), jnp.bfloat16),
        ),
        in_specs=[smem()] + vmem(24),
        out_specs=tuple(vmem(2)),
        scratch_shapes=[
            pltpu.VMEM((Y * tokens, 2 * depth), jnp.bfloat16),
            pltpu.VMEM((2 * depth, Z * BLOCK), jnp.bfloat16),
        ],
        cost_estimate=pl.CostEstimate(
            flops=2 * Y * tokens * 2 * depth * Z * BLOCK, bytes_accessed=1 << 23, transcendentals=0
        ),
        name="project",
    )(slots, *acts_own, *acts_other, *w_own, *w_other)


def hidden_kernel(turn_ref, resid_ref, b0, b1, b2, b3, hidden_ref, square_ref):
    tokens = resid_ref.shape[0]
    total = jnp.zeros((tokens, BLOCK), jnp.float32)
    for j, block in enumerate((b0, b1, b2, b3)):
        for zl in range(Z // 2):
            cols = pl.ds(pl.multiple_of((zl * Y + turn_ref[j]) * BLOCK, BLOCK), BLOCK)
            value = (
                resid_ref[:, cols].astype(jnp.float32)
                + block[:, zl * BLOCK : (zl + 1) * BLOCK].astype(jnp.float32)
            ).astype(jnp.bfloat16)
            hidden_ref[:, cols] = value
            wide = value.astype(jnp.float32)
            total = total + wide * wide
    row = jnp.sum(jnp.transpose(total), axis=0, keepdims=True)
    square_ref[...] = jnp.broadcast_to(row, square_ref.shape)


def make_hidden(turns, resid, blocks):
    tokens, cols = resid.shape
    return pl.pallas_call(
        hidden_kernel,
        out_shape=(
            jax.ShapeDtypeStruct((tokens, cols), jnp.bfloat16),
            jax.ShapeDtypeStruct((8, tokens), jnp.float32),
        ),
        in_specs=[smem()] + vmem(5),
        out_specs=tuple(vmem(2)),
        cost_estimate=pl.CostEstimate(flops=1 << 22, bytes_accessed=1 << 21, transcendentals=0),
        name="hidden",
    )(turns, resid, *blocks)


def norm_kernel(hidden_ref, gain_ref, s0, s1, s2, s3, out_ref, *, wide_cols):
    tokens, cols = hidden_ref.shape
    total = (s0[0:1, :] + s1[0:1, :]) + (s2[0:1, :] + s3[0:1, :])
    scale = lax.rsqrt(total / wide_cols + 1e-05)
    scale = jnp.transpose(jnp.broadcast_to(scale, (BLOCK, tokens)))
    for c in range(0, cols, BLOCK):
        value = hidden_ref[:, c : c + BLOCK].astype(jnp.float32)
        out_ref[:, c : c + BLOCK] = (value * gain_ref[:, c : c + BLOCK] * scale).astype(jnp.bfloat16)


def make_normed(hidden, gain, squares, wide_cols):
    def body(*refs):
        norm_kernel(*refs, wide_cols=wide_cols)

    return pl.pallas_call(
        body,
        out_shape=jax.ShapeDtypeStruct(hidden.shape, jnp.bfloat16),
        in_specs=vmem(6),
        out_specs=vmem(1)[0],
        cost_estimate=pl.CostEstimate(flops=1 << 21, bytes_accessed=1 << 21, transcendentals=0),
        name="normed",
    )(hidden, gain.reshape(1, -1), *squares)


def on_device(attn_out, w_blocks, w_scales, residual, gain):
    dp, tensor = lax.axis_index("dp"), lax.axis_index("tensor")
    xl, z, y = dp // (Z * Y), (dp // Y) % Z, dp % Y
    xh, core = tensor // 2, tensor % 2
    my_cols = gain.shape[0]

    mine = dequantize(w_blocks, w_scales)
    first = move(mine, lambda xl, z, y, xh, c: (1 - xl, z, y, xh, c) if xh == xl else (xl, z, y, 1 - xh, c))
    second = move(mine, lambda xl, z, y, xh, c: None if xh == xl else (1 - xl, z, y, 1 - xh, c))
    straight = xl == xh
    own = {0: jnp.where(straight, mine, first)}
    other = {0: jnp.where(straight, first, second)}

    acts_own = {0: attn_out}
    acts_other = {0: move(attn_out, lambda xl, z, y, xh, c: (xl, z, y, 1 - xh, c))}
    for j in (1, 3, 2):
        acts_own[j] = move(acts_own[0], lambda xl, z, y, xh, c: (xl, z, y - j, xh, c))
    for j in (1, 3, 2):
        acts_other[j] = move(acts_other[0], lambda xl, z, y, xh, c: (xl, z, y - j, xh, c))

    def down(x):
        return move(x, lambda xl, z, y, xh, c: (xl, z - 1, y, xh, c))

    def up(x):
        return move(x, lambda xl, z, y, xh, c: (xl, z + 1, y, xh, c))

    for k in range(1, 4):
        own[k], own[-k] = down(own[k - 1]), up(own[1 - k])
        other[k], other[-k] = down(other[k - 1]), up(other[1 - k])
    own[4], other[4] = down(own[3]), up(other[-3])

    order = [0, 1, -1, 2, -2, 3, -3, 4]
    held = (z + jnp.array([k % Z for k in order], jnp.int32)) % Z
    slots = jnp.where(held // 4 == core, 0, 4) + held % 4
    keep, send = project(
        slots,
        [acts_own[j] for j in range(Y)],
        [acts_other[j] for j in range(Y)],
        [own[k] for k in order],
        [other[k] for k in order],
    )
    came = move(send, lambda xl, z, y, xh, c: (xl, z, y, xh, 1 - c))
    tokens = attn_out.shape[0]
    tiles = []
    for j in range(Y):
        rows = slice(j * tokens, (j + 1) * tokens)
        tiles.append((keep[rows] + came[rows].astype(jnp.float32)).astype(jnp.bfloat16))
    blocks = [tiles[0]]
    for j in range(1, Y):
        blocks.append(move(tiles[j], lambda xl, z, y, xh, c: (xl, z, y + j, xh, c)))

    resid = lax.dynamic_slice_in_dim(residual, tensor * my_cols, my_cols, 1)
    turns = (y - jnp.arange(Y, dtype=jnp.int32)) % Y
    hidden, square = make_hidden(turns, resid, blocks)
    squares = [
        square,
        move(square, lambda xl, z, y, xh, c: (xl, z, y, xh, 1 - c)),
        move(square, lambda xl, z, y, xh, c: (xl, z, y, 1 - xh, c)),
        move(square, lambda xl, z, y, xh, c: (xl, z, y, 1 - xh, 1 - c)),
    ]
    normed = make_normed(hidden, gain, squares, residual.shape[1])
    return (hidden, normed)


def solution(mesh):
    return jax.shard_map(
        on_device,
        mesh=mesh,
        in_specs=(
            P("dp", "tensor"),
            P("tensor", "dp"),
            P("tensor", "dp"),
            P("dp", None),
            P("tensor"),
        ),
        out_specs=(P("dp", "tensor"), P("dp", "tensor")),
        check_vma=False,
    )
```

```python
import functools

import jax
import jax.numpy as jnp
from jax import lax
from jax.experimental import pallas as pl
from jax.experimental.pallas import tpu as pltpu
from jax.sharding import PartitionSpec as P


BLOCK = 128
XL, Z, Y, XH, CORE = 2, 8, 4, 2, 2
EARLY, LATE = (2, 1, 3), (0,)


def move(x, where):
    pairs = []
    for xl in range(XL):
        for z in range(Z):
            for y in range(Y):
                for xh in range(XH):
                    for core in range(CORE):
                        to = where(xl, z, y, xh, core)
                        if to is None:
                            continue
                        xl2, z2, y2, xh2, core2 = to
                        source = ((xl * Z + z) * Y + y) * 4 + xh * 2 + core
                        target = ((xl2 * Z + z2 % Z) * Y + y2 % Y) * 4 + xh2 * 2 + core2
                        pairs.append((source, target))
    return lax.ppermute(x, ("dp", "tensor"), pairs)


def dequantize(blocks, scales):
    rows, cols = blocks.shape
    shaped = blocks.astype(jnp.float32).reshape(rows // BLOCK, BLOCK, cols)
    return (shaped * scales[:, None, :]).reshape(rows, cols).astype(jnp.bfloat16)


def vmem(count):
    return [pl.BlockSpec(memory_space=pltpu.VMEM)] * count


def position():
    return lax.rem(lax.div(lax.axis_index("dp"), Y), Z), lax.rem(lax.axis_index("tensor"), CORE)


def project_kernel(pairs, acts_ref, *refs):
    count = len(pairs)
    w_own, w_other = refs[0 : 2 * count], refs[2 * count : 4 * count]
    keep_ref, send_ref, weights = refs[4 * count :]
    depth = w_own[0].shape[0]
    width = count * BLOCK

    @pl.when(pl.program_id(0) == 0)
    def _():
        z, core = position()
        for p in range(count):
            for i in range(2):
                held = lax.rem(z + (pairs[p] + 4 * i) % Z, Z)
                kept = lax.div(held, Z // 2) == core
                start = jnp.where(kept, 0, width) + p * BLOCK
                cols = pl.ds(pl.multiple_of(start, BLOCK), BLOCK)
                weights[0:depth, cols] = w_own[2 * p + i][...]
                weights[depth : 2 * depth, cols] = w_other[2 * p + i][...]

    sums = jnp.dot(acts_ref[...], weights[...], preferred_element_type=jnp.float32)
    keep_ref[...] = sums[:, :width]
    send_ref[...] = sums[:, width:].astype(jnp.bfloat16)


def project(pairs, acts, own, other):
    rows, features = acts.shape
    tokens, count = rows // Y, len(pairs)
    width = count * BLOCK
    order = [k for p in pairs for k in (p, p - 4)]
    blocks = [own[k] for k in order] + [other[k] for k in order]
    return pl.pallas_call(
        functools.partial(project_kernel, pairs),
        grid=(Y,),
        out_shape=(
            jax.ShapeDtypeStruct((rows, width), jnp.float32),
            jax.ShapeDtypeStruct((rows, width), jnp.bfloat16),
        ),
        in_specs=[pl.BlockSpec((tokens, features), lambda j: (j, 0))]
        + [pl.BlockSpec(block.shape, lambda j: (0, 0)) for block in blocks],
        out_specs=(
            pl.BlockSpec((tokens, width), lambda j: (j, 0)),
            pl.BlockSpec((tokens, width), lambda j: (j, 0)),
        ),
        scratch_shapes=[pltpu.VMEM((features, 2 * width), jnp.bfloat16)],
        compiler_params=pltpu.CompilerParams(vmem_limit_bytes=20 << 20),
        cost_estimate=pl.CostEstimate(
            flops=4 * rows * features * width, bytes_accessed=1 << 23, transcendentals=0
        ),
    )(acts, *blocks)


def merge_kernel(*refs):
    out_ref = refs[-1]
    start = 0
    for keep_ref, came_ref in zip(refs[0:-1:2], refs[1:-1:2]):
        width = keep_ref.shape[1]
        out_ref[:, start : start + width] = (
            keep_ref[...] + came_ref[...].astype(jnp.float32)
        ).astype(jnp.bfloat16)
        start += width


def merge_tile(parts, j):
    tokens = parts[0].shape[0] // Y
    cols = sum(part.shape[1] for part in parts[::2])
    return pl.pallas_call(
        merge_kernel,
        grid=(1,),
        out_shape=jax.ShapeDtypeStruct((tokens, cols), jnp.bfloat16),
        in_specs=[pl.BlockSpec((tokens, part.shape[1]), lambda i: (j, 0)) for part in parts],
        out_specs=pl.BlockSpec((tokens, cols), lambda i: (0, 0)),
        compiler_params=pltpu.CompilerParams(vmem_limit_bytes=8 << 20),
        cost_estimate=pl.CostEstimate(flops=1 << 20, bytes_accessed=1 << 20, transcendentals=0),
        name="merge",
    )(*parts)


def hidden_kernel(resid_ref, b0, b1, b2, b3, hidden_ref, again_ref, square_ref):
    tokens = resid_ref.shape[0]
    y = lax.rem(lax.axis_index("dp"), Y)
    z, _ = position()
    total = jnp.zeros((tokens, BLOCK), jnp.float32)
    for j, block in enumerate((b0, b1, b2, b3)):
        for i, k in enumerate(EARLY + LATE):
            zl = lax.rem(z + k, Z // 2)
            at = zl * Y + lax.rem(y + (Y - j), Y)
            cols = pl.ds(pl.multiple_of(at * BLOCK, BLOCK), BLOCK)
            value = (
                resid_ref[:, cols].astype(jnp.float32)
                + block[:, i * BLOCK : (i + 1) * BLOCK].astype(jnp.float32)
            ).astype(jnp.bfloat16)
            hidden_ref[:, cols] = value
            again_ref[:, cols] = value
            wide = value.astype(jnp.float32)
            total = total + wide * wide
    row = jnp.sum(jnp.transpose(total), axis=0, keepdims=True)
    square_ref[...] = jnp.broadcast_to(row, square_ref.shape)


def make_hidden(resid, blocks):
    tokens, cols = resid.shape
    return pl.pallas_call(
        hidden_kernel,
        out_shape=(
            jax.ShapeDtypeStruct((tokens, cols), jnp.bfloat16),
            jax.ShapeDtypeStruct((tokens, cols), jnp.bfloat16),
            jax.ShapeDtypeStruct((8, tokens), jnp.float32),
        ),
        in_specs=vmem(5),
        out_specs=tuple(vmem(3)),
        cost_estimate=pl.CostEstimate(flops=1 << 22, bytes_accessed=1 << 21, transcendentals=0),
        compiler_params=pltpu.CompilerParams(vmem_limit_bytes=16 << 20),
        name="hidden",
    )(resid, *blocks)


def norm_kernel(hidden_ref, gain_ref, s0, s1, s2, s3, out_ref, *, wide_cols):
    tokens, cols = hidden_ref.shape
    total = (s0[0:1, :] + s1[0:1, :]) + (s2[0:1, :] + s3[0:1, :])
    scale = lax.rsqrt(total / wide_cols + 1e-05)
    scale = jnp.transpose(jnp.broadcast_to(scale, (BLOCK, tokens)))
    for c in range(0, cols, BLOCK):
        value = hidden_ref[:, c : c + BLOCK].astype(jnp.float32)
        out_ref[:, c : c + BLOCK] = (value * gain_ref[:, c : c + BLOCK] * scale).astype(jnp.bfloat16)


def make_normed(again, gain, squares, wide_cols):
    def body(*refs):
        norm_kernel(*refs, wide_cols=wide_cols)

    return pl.pallas_call(
        body,
        out_shape=jax.ShapeDtypeStruct(again.shape, jnp.bfloat16),
        in_specs=vmem(6),
        out_specs=vmem(1)[0],
        cost_estimate=pl.CostEstimate(flops=1 << 21, bytes_accessed=1 << 21, transcendentals=0),
        compiler_params=pltpu.CompilerParams(vmem_limit_bytes=16 << 20),
        name="normed",
    )(again, gain.reshape(1, -1), *squares)


def on_device(attn_out, w_blocks, w_scales, residual, gain):
    tensor = lax.axis_index("tensor")
    my_cols = gain.shape[0]

    mine = dequantize(w_blocks, w_scales)
    first = move(mine, lambda xl, z, y, xh, c: (1 - xl, z, y, xh, c) if xh == xl else None)
    second = move(mine, lambda xl, z, y, xh, c: None if xh == xl else (1 - xl, z, y, 1 - xh, c))
    third = move(second, lambda xl, z, y, xh, c: None if xh == xl else (1 - xl, z, y, xh, c))
    straight = lax.div(lax.axis_index("dp"), Z * Y) == lax.div(tensor, CORE)
    own = {0: jnp.where(straight, mine, first)}
    other = {0: jnp.where(straight, third, second)}

    acts_own = {0: attn_out}
    for j in (1, 3, 2):
        acts_own[j] = move(attn_out, lambda xl, z, y, xh, c: (xl, z, y - j, xh, c))
    across = lambda xl, z, y, xh, c: (xl, z, y, 1 - xh, c)
    acts_other = {0: move(attn_out, across), 2: move(acts_own[2], across)}
    for j in (1, 3):
        acts_other[j] = move(acts_other[0], lambda xl, z, y, xh, c: (xl, z, y - j, xh, c))

    def down(x):
        return move(x, lambda xl, z, y, xh, c: (xl, z - 1, y, xh, c))

    def up(x):
        return move(x, lambda xl, z, y, xh, c: (xl, z + 1, y, xh, c))

    for k in range(1, 4):
        own[k], own[-k] = down(own[k - 1]), up(own[1 - k])
        other[k], other[-k] = down(other[k - 1]), up(other[1 - k])
    own[-4], other[-4] = down(own[3]), up(other[-3])

    acts = jnp.concatenate(
        [jnp.concatenate([acts_own[j], acts_other[j]], axis=1) for j in range(Y)], axis=0
    )
    parts = []
    for pairs in (EARLY, LATE):
        keep, send = project(pairs, acts, own, other)
        parts += [keep, move(send, lambda xl, z, y, xh, c: (xl, z, y, xh, 1 - c))]
    blocks = {}
    for j in (2, 1, 3):
        blocks[j] = move(merge_tile(parts, j), lambda xl, z, y, xh, c: (xl, z, y + j, xh, c))
    blocks[0] = merge_tile(parts, 0)

    resid = lax.dynamic_slice_in_dim(residual, tensor * my_cols, my_cols, 1)
    hidden, again, square = make_hidden(resid, [blocks[j] for j in range(Y)])
    squares = [
        square,
        move(square, lambda xl, z, y, xh, c: (xl, z, y, 1 - xh, 1 - c)),
        move(square, lambda xl, z, y, xh, c: (xl, z, y, 1 - xh, c)),
        move(square, lambda xl, z, y, xh, c: (xl, z, y, xh, 1 - c)),
    ]
    normed = make_normed(again, gain, squares, residual.shape[1])
    return (hidden, normed)


def solution(mesh):
    return jax.shard_map(
        on_device,
        mesh=mesh,
        in_specs=(
            P("dp", "tensor"),
            P("tensor", "dp"),
            P("tensor", "dp"),
            P("dp", None),
            P("tensor"),
        ),
        out_specs=(P("dp", "tensor"), P("dp", "tensor")),
        check_vma=False,
    )
```
